32 devices in a mesh: grp: 4 (over x, core), pages: 8 (over z, y).
Axes of the slice: x: 2, y: 2, z: 4, core: 2. Of those that a mesh axis runs over, the one named last changes fastest.
Arguments:
- queries: bfloat16 [128, 64, 2048], P(('grp', 'pages')), parts along dimension 0, may hold values from -500 to 500
- tree_keys: bfloat16 [128, 64, 512], P(('grp', 'pages')), parts along dimension 0, may hold values from -6 to 6
- tree_values: bfloat16 [128, 64, 512], P(('grp', 'pages')), parts along dimension 0, may hold values from -6 to 6
- page_keys: bfloat16 [256, 256, 512], P(('grp', 'pages')), parts along dimension 0, may hold values from -6 to 6
- page_values: bfloat16 [256, 256, 512], P(('grp', 'pages')), parts along dimension 0, may hold values from -6 to 6
- page_table: int32 [128, 4], P(('grp', 'pages')), parts along dimension 0, may hold values from 0 to 63, as said below
- prefix_lengths: int32 [128], P(('grp', 'pages')), parts along dimension 0, may hold values from 513 to 1024
- tree_parents: int32 [128, 64], P(('grp', 'pages')), parts along dimension 0, may hold values from -1 to 62, as said below
- live_lengths: int32 [128], P(('grp', 'pages')), parts along dimension 0, may hold values from 1 to 64
Outputs:
- attended: bfloat16 [128, 64, 2048], P(('grp', 'pages')), parts along dimension 0
- page_reads: int32 [256], P(('grp', 'pages')), parts along dimension 0
The draws below stay inside these ranges and needn't reach their ends.
There are 4 independent parts, one for each index of `grp`. The reference program is written for one: setup_inputs(seed, part) draws one part's arguments, and reference() takes and returns one part's arrays. A program takes and returns all parts, laid end to end along the dimension named above; each array names one. Nothing has to cross between parts.
Inputs may be any that keep to these rules, and one draw needn't show every extreme that they name: `page_table`: the owner of page p is index p // 8 along pages. Over the rows of one device, the used slots name pages of any one owner at most 2 times, and in every draw each device names some owner exactly 2 times. `tree_parents`: entry t is -1 for t = 0 and a number below t otherwise.
All inputs are finite; a program needn't handle non-finite values.
Results may differ from the reference program's by a relative error of at most 0.0085.
Values may be sent and summed in bfloat16 or wider, within the bound.
A program may use at most 192 MiB of HBM per device.

```python
import jax
import jax.numpy as jnp
from jax import lax

QH = 16
KVH = 4
HD = 128
TREE = 64
PAGE = 256
MAXP = 4
REQ_DEV = 4
PAGES_DEV = 8
REQ = 32
NPAGES = 64
CAP = 2


def draw_queries(key, part):
    first = jax.random.fold_in(key, 0)
    fourth = jax.random.fold_in(key, 3)
    base = jnp.clip(jax.random.normal(first, (REQ, TREE, QH * HD), jnp.float32), -6.0, 6.0)
    moderate_amount = jnp.exp(jax.random.uniform(fourth, (REQ, TREE, 1), jnp.float32, jnp.log(0.5), jnp.log(2.0)))
    factor = moderate_amount
    return (base * factor).astype(jnp.bfloat16)


def draw_tree_parents(key, part):
    index = jnp.arange(TREE, dtype=jnp.int32)
    upper = jnp.maximum(index, 1)
    parents = jax.random.randint(key, (REQ, TREE), 0, upper[None, :], jnp.int32)
    return jnp.where(index[None, :] == 0, -1, parents).astype(jnp.int32)


def draw_page_table(key, part):
    every_owner_list = REQ // REQ_DEV
    choose = REQ_DEV * MAXP // CAP
    key_hot, key_score, key_page = jax.random.split(jax.random.fold_in(key, 7), 3)
    sorted_ranking = jax.random.permutation(key_hot, every_owner_list)
    popular_page_count = max(1, every_owner_list // 8)
    extra_reward = jnp.where(sorted_ranking < popular_page_count, 1 << 24, 0).astype(jnp.int32)
    random_jitter = jax.random.randint(key_score, (every_owner_list, every_owner_list), 0, 4096, jnp.int32)
    score_values = random_jitter * every_owner_list + jnp.arange(every_owner_list, dtype=jnp.int32)[None, :] + extra_reward[None, :]
    chosen = lax.top_k(score_values, choose)[1].astype(jnp.int32)
    local_req = jnp.arange(REQ_DEV, dtype=jnp.int32)
    slot = jnp.arange(MAXP, dtype=jnp.int32)
    group = (slot[None, :] * REQ_DEV + local_req[:, None]) // CAP
    owner = chosen[:, group].reshape(REQ, MAXP)
    local = jax.random.randint(key_page, (REQ, MAXP), 0, PAGES_DEV, jnp.int32)
    return (owner * PAGES_DEV + local).astype(jnp.int32)


def with_ends(drawn, own_key, low, high):
    index_at = [jax.random.randint(jax.random.fold_in(own_key, axis), (), 0, length) for axis, length in enumerate(drawn.shape)]
    main_axis = drawn.shape.index(max(drawn.shape))
    neighbour = index_at[:main_axis] + [(index_at[main_axis] + 1) % drawn.shape[main_axis]] + index_at[main_axis + 1:]
    return drawn.at[tuple(index_at)].set(low).at[tuple(neighbour)].set(high)


def shard_levels(own_key, extent, cuts, smallest, largest):
    factor_of = 1.0
    for position, blocks in cuts:
        draws = jax.random.uniform(jax.random.fold_in(jax.random.fold_in(own_key, 6), position), (blocks,), jnp.float32, smallest / len(cuts), largest / len(cuts))
        factor_of = factor_of * jnp.repeat(jnp.exp(draws), extent[position] // blocks).reshape((-1,) + (1,) * (len(extent) - 1 - position))
    return factor_of


def gaussian(rng, extent, scale, most, pieces=(), held_as=jnp.bfloat16):
    drawn = jax.random.normal(rng, extent, jnp.float32) * scale
    if len(pieces) > 0:
        drawn = shard_levels(rng, extent, pieces, -0.22, 0.18) * drawn
    return jnp.clip(drawn, min=-most, max=most).astype(held_as)


def setup_inputs(seed: int = 0, part: int = 0) -> dict:
    key_list = jax.random.split(jax.random.key(seed), 10)
    own_keys = jax.random.split(jax.random.fold_in(key_list[9], part), 10)
    return {
        "queries": draw_queries(jax.random.fold_in(jax.random.fold_in(key_list[9], part), 71), part),
        "tree_keys": gaussian(own_keys[1], (REQ, TREE, KVH * HD), 1.0, 6.0, ((0, 8),)),
        "tree_values": gaussian(own_keys[2], (REQ, TREE, KVH * HD), 1.0, 6.0, ((0, 8),)),
        "page_keys": gaussian(own_keys[3], (NPAGES, PAGE, KVH * HD), 1.0, 6.0, ((0, 8),)),
        "page_values": gaussian(own_keys[4], (NPAGES, PAGE, KVH * HD), 1.0, 6.0, ((0, 8),)),
        "page_table": draw_page_table(jax.random.fold_in(jax.random.fold_in(key_list[9], part), 71), part),
        "prefix_lengths": with_ends(jax.random.randint(own_keys[6], (REQ,), (MAXP // 2) * PAGE + 1, MAXP * PAGE + 1), jax.random.fold_in(own_keys[6], 1), (MAXP // 2) * PAGE + 1, MAXP * PAGE).astype(jnp.int32),
        "tree_parents": draw_tree_parents(jax.random.fold_in(jax.random.fold_in(key_list[9], part), 71), part),
        "live_lengths": with_ends(jax.random.randint(own_keys[8], (REQ,), 1, TREE + 1), jax.random.fold_in(own_keys[8], 1), 1, TREE).astype(jnp.int32),
    }


NEG_BIG = -1e30


def ancestry(parents):
    index = jnp.arange(TREE, dtype=jnp.int32)
    links = (index[None, None, :] == parents[:, :, None]) | (index[None, :, None] == index[None, None, :])
    reach = links.astype(jnp.float32)
    for level in range((TREE - 1).bit_length()):
        reach = (jnp.einsum("rts,rsu->rtu", reach, reach, precision=lax.Precision.HIGHEST) > 0).astype(jnp.float32)
    return reach


def tree_parts(queries, keys, values, reach, live):
    groups = QH // KVH
    count = queries.shape[0]
    query = queries.astype(jnp.float32).reshape(count, TREE, KVH, groups, HD)
    keyed = keys.astype(jnp.float32).reshape(count, TREE, KVH, HD)
    valued = values.astype(jnp.float32).reshape(count, TREE, KVH, HD)
    score_values = jnp.einsum("rtkgd,rskd->rkgts", query, keyed, precision=lax.Precision.HIGHEST) * HD ** -0.5
    allowed = (reach > 0) & (jnp.arange(TREE, dtype=jnp.int32)[None, None, :] < live[:, None, None])
    score_values = jnp.where(allowed[:, None, None, :, :], score_values, NEG_BIG)
    peak = jnp.max(score_values, axis=-1)
    expo = jnp.exp(score_values - peak[..., None])
    total = jnp.sum(expo, axis=-1)
    weights = lax.optimization_barrier(expo.astype(jnp.bfloat16)).astype(jnp.float32)
    out = jnp.einsum("rkgts,rskd->rtkgd", weights, valued, precision=lax.Precision.HIGHEST)
    out = out.reshape(count, TREE, QH, HD)
    peak = peak.transpose(0, 3, 1, 2).reshape(count, TREE, QH)
    total = total.transpose(0, 3, 1, 2).reshape(count, TREE, QH)
    return peak, total, out


def page_parts(query_rows, keys, values, counts):
    groups = QH // KVH
    query = query_rows.astype(jnp.float32).reshape(TREE, KVH, groups, HD)
    keyed = keys.astype(jnp.float32).reshape(MAXP, PAGE, KVH, HD)
    valued = values.astype(jnp.float32).reshape(MAXP, PAGE, KVH, HD)
    score_values = jnp.einsum("tkgd,jpkd->jkgtp", query, keyed, precision=lax.Precision.HIGHEST) * HD ** -0.5
    allowed = jnp.arange(PAGE, dtype=jnp.int32)[None, :] < counts[:, None]
    score_values = jnp.where(allowed[:, None, None, None, :], score_values, NEG_BIG)
    peak = jnp.max(score_values, axis=-1)
    expo = jnp.exp(score_values - peak[..., None])
    total = jnp.sum(expo, axis=-1)
    weights = lax.optimization_barrier(expo.astype(jnp.bfloat16)).astype(jnp.float32)
    out = jnp.einsum("jkgtp,jpkd->jtkgd", weights, valued, precision=lax.Precision.HIGHEST)
    out = out.astype(jnp.bfloat16).reshape(MAXP, TREE, QH, HD)
    peak = peak.transpose(0, 3, 1, 2).reshape(MAXP, TREE, QH)
    total = total.transpose(0, 3, 1, 2).reshape(MAXP, TREE, QH)
    return peak, total, out


def reference(queries, tree_keys, tree_values, page_keys, page_values, page_table, prefix_lengths, tree_parents, live_lengths):
    slots = jnp.arange(MAXP, dtype=jnp.int32)
    key_counts = jnp.clip(prefix_lengths[:, None] - slots[None, :] * PAGE, 0, PAGE).astype(jnp.int32)
    used = key_counts > 0
    reach = ancestry(tree_parents)
    tree_peak, tree_total, tree_out = tree_parts(queries, tree_keys, tree_values, reach, live_lengths)

    def one_request(items):
        query_rows, table_row, count_row = items
        return page_parts(query_rows, page_keys[table_row], page_values[table_row], count_row)

    page_maximum, page_total, page_out = lax.map(one_request, (queries, page_table, key_counts))
    usable = used[:, :, None, None]
    masked = jnp.where(usable, page_maximum, NEG_BIG)
    top = jnp.maximum(tree_peak, jnp.max(masked, axis=1))
    tree_scale = jnp.exp(tree_peak - top)
    page_scale = jnp.where(usable, jnp.exp(masked - top[:, None]), 0.0)
    total = tree_total * tree_scale + jnp.sum(page_scale * page_total, axis=1)
    mixed = tree_out * tree_scale[..., None] + jnp.sum(page_scale[..., None] * page_out.astype(jnp.float32), axis=1)
    attended = (mixed / total[..., None]).reshape(REQ, TREE, QH * HD).astype(jnp.bfloat16)
    weight = jnp.where(used, live_lengths[:, None], 0).astype(jnp.float32)
    reads = jax.ops.segment_sum(weight.reshape(-1), page_table.reshape(-1), num_segments=NPAGES)
    return attended, reads.astype(jnp.int32)
```

```python
import functools
import heapq
import itertools

import jax
import jax.numpy as jnp
from jax import lax
from jax.experimental import pallas as pl
from jax.experimental.pallas import tpu as pltpu
from jax.sharding import PartitionSpec as P

QH = 16
KVH = 4
HD = 128
GROUPS = QH // KVH
NEG_BIG = -1e30
SCALE = HD ** (-0.5)
NT = (((1,), (1,)), ((), ()))
TN = (((0,), (0,)), ((), ()))
MESH = pl.DeviceIdType.MESH
CHUNKS = 4
GRANT = 63 * 1024 * 1024

PICK, LOCAL, ACROSS, MERGE, Q_RIGHT, Q_LEFT, STATE, Y_QUERY, Y_PART = range(9)


def head(h):
    return slice(h * HD, (h + 1) * HD)


def plan(depth, chunks, start=5.0):
    per = 4.0 / chunks
    wire = {Q_RIGHT: 5.63 * per, Q_LEFT: 5.63 * per, STATE: 5.8 * per}
    wire.update({Y_QUERY: 2.82 * per, Y_PART: 2.9 * per})
    work = {PICK: 0.15 * per, LOCAL: 0.6 * per, ACROSS: 0.6 * per, MERGE: 0.45 * per}
    delay = 1.8
    rank = {PICK: 0, ACROSS: 1, MERGE: 2, LOCAL: 3}
    events, tick = [], itertools.count()
    have = [set() for _ in range(depth)]
    queue, busy, last = {}, {}, {}
    idle = [False] * depth
    todo = [
        {(kind, s, k) for kind in rank for s in range(depth) for k in range(chunks)}
        for _ in range(depth)
    ]
    issued = [[] for _ in range(depth)]

    def post(time, what, *facts):
        heapq.heappush(events, (time, next(tick), what, facts))

    def pump(time, key):
        if busy.get(key) or not queue.get(key):
            return
        _, _, ready, op, tag, dest = heapq.heappop(queue[key])
        busy[key] = True
        issued[key[0]].append((max(ready, last.get(key, 0.0)), 0, next(tick), op))
        last[key] = time
        post(time + wire[op[0]], "free", key)
        post(time + wire[op[0]] + delay, "land", tag, dest)

    def send(time, z, link, op, tag, dest):
        order = (op[0] not in (Q_RIGHT, Q_LEFT, Y_QUERY), -abs(op[1] - z), op[2])
        heapq.heappush(
            queue.setdefault((z, link), []), (order, next(tick), time, op, tag, dest)
        )
        pump(time, (z, link))

    def send_query(time, z, s, k):
        if s <= z < depth - 1:
            send(time, z, "right", (Q_RIGHT, s, k), ("q", s, k), z + 1)
        if s >= z > 0:
            send(time, z, "left", (Q_LEFT, s, k), ("q", s, k), z - 1)

    def ready(z, op):
        kind, s, k = op
        if kind == PICK:
            return s == z or ("q", s, k) in have[z]
        if kind == LOCAL:
            return (PICK, s, k) in have[z]
        if kind == ACROSS:
            return ("yq", s, k) in have[z]
        need = [(LOCAL, s, k), ("yp", s, k)]
        need += [("right", s, k)] * (s >= z and z > 0)
        need += [("left", s, k)] * (s <= z and z < depth - 1)
        return all(n in have[z] for n in need)

    def turn(time, z):
        if not idle[z]:
            return
        able = [op for op in todo[z] if ready(z, op)]
        if not able:
            return
        op = min(able, key=lambda o: (rank[o[0]], -abs(o[1] - z), o[2], o[1]))
        todo[z].remove(op)
        issued[z].append((time, 1, next(tick), op))
        idle[z] = False
        if op[0] == PICK and op[1] != z:
            send_query(time + 1e-3, z, op[1], op[2])
        post(time + work[op[0]], "done", z, op)

    for z in range(depth):
        for k in range(chunks):
            send_query(0.0, z, z, k)
        post(start, "done", z, None)
    while events:
        time, _, what, facts = heapq.heappop(events)
        if what == "free":
            busy[facts[0]] = False
            pump(time, facts[0])
        elif what == "land":
            have[facts[1]].add(facts[0])
            turn(time, facts[1])
        else:
            z, op = facts
            idle[z] = True
            if op is not None:
                kind, s, k = op
                have[z].add(op)
                if kind == PICK:
                    send(time, z, "y", (Y_QUERY, s, k), ("yq", s, k), z)
                elif kind == ACROSS:
                    send(time, z, "y", (Y_PART, s, k), ("yp", s, k), z)
                elif kind == MERGE and s > z:
                    send(time, z, "right", (STATE, s, k), ("right", s, k), z + 1)
                elif kind == MERGE and s < z:
                    send(time, z, "left", (STATE, s, k), ("left", s, k), z - 1)
            turn(time, z)
    items = depth * chunks
    orders = [
        [op[0] * items + op[1] * chunks + op[2] for _, _, _, op in sorted(steps)]
        for steps in issued
    ]
    longest = max(len(o) for o in orders)
    return [o + [-1] * (longest - len(o)) for o in orders]


def attend_part(query, keys, values, allowed):
    scores = lax.dot_general(keys, query, NT, preferred_element_type=jnp.float32) * SCALE
    scores = jnp.where(allowed, scores, NEG_BIG)
    peak = jnp.max(scores, axis=0, keepdims=True)
    expo = jnp.exp(scores - peak)
    total = jnp.sum(expo, axis=0, keepdims=True)
    out = lax.dot_general(
        values, expo.astype(jnp.bfloat16), TN, preferred_element_type=jnp.float32
    )
    return out * (1.0 / total), peak + jnp.log(total)


def chain(
    n,
    cap,
    chunks,
    orders,
    table,
    prefix,
    live,
    parents_ref,
    tk_ref,
    tv_ref,
    q_hbm,
    pk_hbm,
    pv_hbm,
    attended,
    reads_ref,
    pk_ref,
    pv_ref,
    label_ref,
    labels,
    label_now,
    qa,
    q_now,
    yq_send,
    yq_got,
    yo_send,
    yo_got,
    ys_send,
    ys_got,
    loc_o,
    loc_s,
    st_o,
    st_s,
    tree_o,
    tree_s,
    open_ref,
    label_send_sem,
    label_recv_sem,
    q_send_sem,
    q_recv_sem,
    yq_send_sem,
    yq_recv_sem,
    yo_send_sem,
    yo_recv_sem,
    ys_send_sem,
    ys_recv_sem,
    so_send_sem,
    so_recv_sem,
    ss_send_sem,
    ss_recv_sem,
    local_sem,
):
    reqs, tree, wide = q_now.shape
    _, pages_here, page, _ = pk_ref.shape
    slots = table.shape[1]
    depth = n // 2
    items = depth * chunks
    heads = wide // HD
    cols = heads * tree
    tiles = cols // HD
    me = lax.axis_index("pages")
    z, y = me // 2, me % 2
    partner = z * 2 + (1 - y)
    absent = items + chunks

    loads = []
    for k in range(chunks):
        loads.append(
            pltpu.make_async_copy(
                q_hbm.at[:, :, pl.ds(k * wide, wide)],
                qa.at[z * chunks + k],
                local_sem.at[1 + k],
            )
        )
    page_loads = []
    for k in range(KVH):
        for f, (src, dst) in enumerate(((pk_hbm, pk_ref), (pv_hbm, pv_ref))):
            page_loads.append(
                pltpu.make_async_copy(
                    src.at[:, :, pl.ds(k * HD, HD)],
                    dst.at[k],
                    local_sem.at[1 + chunks + 2 * k + f],
                )
            )
    for copy in loads + page_loads:
        copy.start()

    barrier = pltpu.get_barrier_semaphore()

    def greet(i, _):
        pl.semaphore_signal(
            barrier, inc=1, device_id={"pages": (me + i) % n}, device_id_type=MESH
        )
        return 0

    lax.fori_loop(1, n, greet, 0)

    label_row = lax.broadcasted_iota(jnp.int32, (n, HD), 0)
    label_lane = lax.broadcasted_iota(jnp.int32, (n, HD), 1)
    told = jnp.zeros((n, HD), jnp.int32)
    owners, taken = [], []
    for p in range(reqs * slots):
        r, j = p // slots, p % slots
        count = jnp.clip(prefix[r] - j * page, 0, page)
        owner = lax.div(table[r, j], jnp.int32(pages_here))
        rank = jnp.int32(0)
        for earlier in range(p):
            same = (owners[earlier] == owner) & (taken[earlier] > 0)
            rank = rank + jnp.where(same, 1, 0)
        owners.append(owner)
        taken.append(jnp.where(count > 0, 1, 0))
        row = label_row == jnp.where(count > 0, owner, -1)
        facts = (table[r, j] - owner * pages_here, count, r, live[r])
        for f, fact in enumerate(facts):
            told = jnp.where(row & (label_lane == rank * 4 + f), fact, told)
    for d in range(depth):
        label_ref[d, 0:2, :] = told[2 * d : 2 * d + 2]

    base, per_word = 9 * items + 1, 3
    steps = len(orders[0])
    words = []
    for first in range(0, steps, per_word):
        packed = [
            sum((c + 1) * base**b for b, c in enumerate(o[first : first + per_word]))
            for o in orders
        ]
        word = jnp.int32(packed[0])
        for row in range(1, depth):
            if packed[row] != packed[0]:
                word = jnp.where(z == row, packed[row], word)
        words.append(word)

    def code_at(i):
        at, b = i // per_word, i % per_word
        word = words[0]
        for w in range(1, len(words)):
            word = jnp.where(at == w, words[w], word)
        power = jnp.where(b == 0, 1, jnp.where(b == 1, base, base * base))
        return (word // power) % base - 1

    pl.semaphore_wait(barrier, n - 1)

    def label_copy(d):
        return pltpu.make_async_remote_copy(
            src_ref=label_ref.at[d // 2],
            dst_ref=labels.at[me],
            send_sem=label_send_sem.at[d],
            recv_sem=label_recv_sem.at[me],
            device_id={"pages": d},
            device_id_type=MESH,
        )

    def tell(i, _):
        label_copy((me + i) % n).start()
        return 0

    lax.fori_loop(1, n, tell, 0)

    def q_copy(j, way):
        return pltpu.make_async_remote_copy(
            src_ref=qa.at[j],
            dst_ref=qa.at[j],
            send_sem=q_send_sem.at[way, j],
            recv_sem=q_recv_sem.at[j],
            device_id={"pages": me + 2 - 4 * way},
            device_id_type=MESH,
        )

    def across(src, dst, send_sem, recv_sem, j):
        return pltpu.make_async_remote_copy(
            src_ref=src.at[j],
            dst_ref=dst.at[j],
            send_sem=send_sem.at[j],
            recv_sem=recv_sem.at[j],
            device_id={"pages": partner},
            device_id_type=MESH,
        )

    def yq_copy(j):
        return across(yq_send, yq_got, yq_send_sem, yq_recv_sem, j)

    def yo_copy(j):
        return across(yo_send, yo_got, yo_send_sem, yo_recv_sem, j)

    def ys_copy(j):
        return across(ys_send, ys_got, ys_send_sem, ys_recv_sem, j)

    def state_copies(j, row, k):
        left = jnp.where(row < z, 1, 0)
        ends = left * jnp.where(row == z - 1, 1, 0)
        slot = j + ends * (items - row * chunks)
        to = {"pages": me + 2 - 4 * left}
        return (
            pltpu.make_async_remote_copy(
                src_ref=st_o.at[j],
                dst_ref=st_o.at[slot],
                send_sem=so_send_sem.at[j],
                recv_sem=so_recv_sem.at[slot],
                device_id=to,
                device_id_type=MESH,
            ),
            pltpu.make_async_remote_copy(
                src_ref=st_s.at[j],
                dst_ref=st_s.at[slot],
                send_sem=ss_send_sem.at[j],
                recv_sem=ss_recv_sem.at[slot],
                device_id=to,
                device_id_type=MESH,
            ),
        )

    def state_arrive(slot):
        for ref, sem in ((st_o, so_recv_sem), (st_s, ss_recv_sem)):
            pltpu.make_async_remote_copy(
                src_ref=ref.at[slot],
                dst_ref=ref.at[slot],
                send_sem=sem.at[slot],
                recv_sem=sem.at[slot],
                device_id={"pages": partner},
                device_id_type=MESH,
            ).wait_recv()

    for copy in loads:
        copy.wait()

    st_o[absent] = jnp.zeros_like(st_o[absent])
    st_s[absent] = jnp.full(st_s.shape[1:], NEG_BIG, jnp.float32)

    def q_step(i, _):
        code = code_at(i)
        kind, j = code // items, code % items

        @pl.when(kind == Q_RIGHT)
        def _():
            q_copy(j, 0).start()

        @pl.when(kind == Q_LEFT)
        def _():
            q_copy(j, 1).start()

        return 0

    early = 0
    while all(o[early] // items in (Q_RIGHT, Q_LEFT) for o in orders):
        early += 1
    lax.fori_loop(0, early, q_step, 0)

    def rows_of(query):
        return jnp.concatenate([query[:, head(h)] for h in range(heads)], axis=0)

    def put_row(ref, index, first, vector):
        for i in range(tiles):
            ref[index, first + i : first + i + 1, :] = vector[:, head(i)]

    def get_row(tile, first):
        return jnp.concatenate(
            [tile[first + i : first + i + 1, :] for i in range(tiles)], axis=1
        )

    source = lax.broadcasted_iota(jnp.int32, (tree, tree), 0)
    child = lax.broadcasted_iota(jnp.int32, (tree, tree), 1)
    reaches = []
    for r in range(reqs):
        linked = (source == parents_ref[r : r + 1, :]) | (source == child)
        reaches.append(jnp.where(linked, 1.0, 0.0).astype(jnp.bfloat16))
    for level in range((tree - 1).bit_length()):
        reaches = [
            jnp.where(
                jnp.dot(reach, reach, preferred_element_type=jnp.float32) > 0, 1.0, 0.0
            ).astype(jnp.bfloat16)
            for reach in reaches
        ]
    for r in range(reqs):
        open_ = jnp.where(source < live[r], reaches[r].astype(jnp.float32), 0.0)
        open_ref[r] = jnp.concatenate([open_] * heads, axis=1)

    def tree_step(k, _):
        kv = k * heads // GROUPS
        lanes = pl.ds(pl.multiple_of(kv * HD, HD), HD)
        for r in range(reqs):
            out, lse = attend_part(
                rows_of(qa[z * chunks + k, r]),
                tk_ref[r, :, lanes],
                tv_ref[r, :, lanes],
                open_ref[r] > 0,
            )
            tree_o[k, r] = out
            put_row(tree_s, k, r * tiles, lse)
        return 0

    lax.fori_loop(0, chunks, tree_step, 0)

    labels[me] = label_ref[z]

    def hear(i, _):
        d = (me + i) % n
        pltpu.make_async_remote_copy(
            src_ref=label_ref.at[d // 2],
            dst_ref=labels.at[d],
            send_sem=label_send_sem.at[d],
            recv_sem=label_recv_sem.at[d],
            device_id={"pages": d},
            device_id_type=MESH,
        ).wait()
        return 0

    lax.fori_loop(1, n, hear, 0)
    into_scalars = pltpu.make_async_copy(labels, label_now, local_sem.at[0])
    into_scalars.start()
    into_scalars.wait()
    for copy in page_loads:
        copy.wait()

    key_row = lax.broadcasted_iota(jnp.int32, (page, cols), 0)

    def serve(d, k, query_of, out_ref, stat_ref, j):
        kv = k * heads // GROUPS
        for c in range(cap):
            which, count, req = (label_now[d, y, c * 4 + f] for f in range(3))
            out, lse = attend_part(
                rows_of(query_of(c, req)),
                pk_ref[kv, which],
                pv_ref[kv, which],
                key_row < count,
            )
            out_ref[j, c] = out.astype(jnp.bfloat16)
            put_row(stat_ref, j, c * tiles, lse)

    def pick(j, row, k):
        @pl.when(row != z)
        def _():
            pltpu.make_async_remote_copy(
                src_ref=qa.at[j],
                dst_ref=qa.at[j],
                send_sem=q_send_sem.at[0, j],
                recv_sem=q_recv_sem.at[j],
                device_id={"pages": partner},
                device_id_type=MESH,
            ).wait_recv()

        q_now[...] = qa[j]
        for c in range(cap):
            yq_send[j, c] = q_now[label_now[row * 2 + y, 1 - y, c * 4 + 2]]

    def local(j, row, k):
        q_now[...] = qa[j]
        serve(row * 2 + y, k, lambda c, req: q_now[req], loc_o, loc_s, j)

    def from_partner(j, row, k):
        yq_copy(j).wait_recv()
        serve(row * 2 + (1 - y), k, lambda c, req: yq_got[j, c], yo_send, ys_send, j)

    def merged(j, row, r, others):
        parts, weights = [], []
        for held_o, held_s, owner in ((loc_o, loc_s, y), (yo_got, ys_got, 1 - y)):
            tile = held_s[j]
            for c in range(cap):
                count, req = (label_now[row * 2 + y, owner, c * 4 + f] for f in (1, 2))
                mine = (count > 0) & (req == r)
                parts.append(held_o[j, c].astype(jnp.float32))
                weights.append(jnp.where(mine, get_row(tile, c * tiles), NEG_BIG))
        for part, lse in others:
            parts.append(part)
            weights.append(lse)
        top = functools.reduce(jnp.maximum, weights)
        weights = [jnp.exp(w - top) for w in weights]
        total = functools.reduce(jnp.add, weights)
        rest = 1.0 / total
        out = parts[0] * (weights[0] * rest)
        for part, weight in zip(parts[1:], weights[1:]):
            out = out + part * (weight * rest)
        return out, top + jnp.log(total)

    def state_part(slot, r):
        return st_o[slot, r].astype(jnp.float32), get_row(st_s[slot], r * tiles)

    def merge(j, row, k):
        yo_copy(j).wait_recv()
        ys_copy(j).wait_recv()

        @pl.when(row != z)
        def _():
            comes = jnp.where(
                row > z, jnp.where(z > 0, 1, 0), jnp.where(z < depth - 1, 1, 0)
            )
            slot = absent + comes * (j - absent)

            @pl.when(comes == 1)
            def _():
                state_arrive(j)

            for r in range(reqs):
                out, lse = merged(j, row, r, [state_part(slot, r)])
                st_o[j, r] = out.astype(jnp.bfloat16)
                put_row(st_s, j, r * tiles, lse)

        @pl.when(row == z)
        def _():
            right = absent + jnp.where(z > 0, 1, 0) * (j - absent)
            left = absent + jnp.where(z < depth - 1, 1, 0) * (items + k - absent)

            @pl.when(z > 0)
            def _():
                state_arrive(j)

            @pl.when(z < depth - 1)
            def _():
                state_arrive(items + k)

            for r in range(reqs):
                own = tree_o[k, r], get_row(tree_s[k], r * tiles)
                out, _ = merged(
                    j, row, r, [state_part(right, r), state_part(left, r), own]
                )
                upright = out.T.astype(jnp.bfloat16)
                for h in range(heads):
                    lanes = pl.ds(pl.multiple_of(k * wide + h * HD, HD), HD)
                    attended[r, :, lanes] = upright[h * tree : (h + 1) * tree]

    def step(i, _):
        code = code_at(i)
        kind, j = code // items, code % items
        row, k = j // chunks, j % chunks

        @pl.when((kind >= 0) & (kind < Q_RIGHT))
        def _():
            @pl.when(kind < ACROSS)
            def _():
                @pl.when(kind == PICK)
                def _():
                    pick(j, row, k)

                @pl.when(kind == LOCAL)
                def _():
                    local(j, row, k)

            @pl.when(kind >= ACROSS)
            def _():
                @pl.when(kind == ACROSS)
                def _():
                    from_partner(j, row, k)

                @pl.when(kind == MERGE)
                def _():
                    merge(j, row, k)

        @pl.when(kind >= Q_RIGHT)
        def _():
            @pl.when(kind < STATE)
            def _():
                @pl.when(kind == Q_RIGHT)
                def _():
                    q_copy(j, 0).start()

                @pl.when(kind == Q_LEFT)
                def _():
                    q_copy(j, 1).start()

            @pl.when(kind == STATE)
            def _():
                for copy in state_copies(j, row, k):
                    copy.start()

            @pl.when(kind == Y_QUERY)
            def _():
                yq_copy(j).start()

            @pl.when(kind == Y_PART)
            def _():
                yo_copy(j).start()
                ys_copy(j).start()

        return 0

    lax.fori_loop(early, len(orders[0]), step, 0)

    page_row = lax.broadcasted_iota(jnp.int32, (pages_here, HD), 0)

    def count_reads(d, reads):
        for c in range(cap):
            which, count, _, lives = (label_now[d, y, c * 4 + f] for f in range(4))
            lives = jnp.where(count > 0, lives, 0)
            reads = reads + jnp.where(page_row == which, lives, 0)
        return reads

    reads_ref[...] = lax.fori_loop(
        0, n, count_reads, jnp.zeros((pages_here, HD), jnp.int32)
    )

    def drain(j, _):
        row, k = j // chunks, j % chunks
        yq_copy(j).wait_send()
        yo_copy(j).wait_send()
        ys_copy(j).wait_send()

        @pl.when((row <= z) & (z < depth - 1))
        def _():
            q_copy(j, 0).wait_send()

        @pl.when((row >= z) & (z > 0))
        def _():
            q_copy(j, 1).wait_send()

        @pl.when(row != z)
        def _():
            for copy in state_copies(j, row, k):
                copy.wait_send()

        return 0

    lax.fori_loop(0, items, drain, 0)


def chain_call(n, cap, args):
    queries, tree_keys, tree_values, page_keys, page_values = args[:5]
    page_table, prefix_lengths, tree_parents, live_lengths = args[5:]
    reqs, tree, width = queries.shape
    pages_here, page, _ = page_keys.shape
    chunks, depth = CHUNKS, n // 2
    items = depth * chunks
    wide = width // chunks
    cols = wide // HD * tree
    tall = max(8, max(reqs, cap) * cols // HD)
    bf16, f32 = jnp.bfloat16, jnp.float32
    dma = pltpu.SemaphoreType.DMA
    smem = pl.BlockSpec(memory_space=pltpu.SMEM)
    vmem = pl.BlockSpec(memory_space=pltpu.VMEM)
    hbm = pl.BlockSpec(memory_space=pl.ANY)
    orders = plan(depth, chunks)
    vmem_scratch = [
        ((KVH, pages_here, page, HD), bf16),
        ((KVH, pages_here, page, HD), bf16),
        ((depth, 8, HD), jnp.int32),
        ((n, 8, HD), jnp.int32),
        None,
        ((items, reqs, tree, wide), bf16),
        ((reqs, tree, wide), bf16),
        ((items, cap, tree, wide), bf16),
        ((items, cap, tree, wide), bf16),
        ((items, cap, HD, cols), bf16),
        ((items, cap, HD, cols), bf16),
        ((items, tall, HD), f32),
        ((items, tall, HD), f32),
        ((items, cap, HD, cols), bf16),
        ((items, tall, HD), f32),
        ((items + chunks + 1, reqs, HD, cols), bf16),
        ((items + chunks + 1, tall, HD), f32),
        ((chunks, reqs, HD, cols), f32),
        ((chunks, tall, HD), f32),
        ((reqs, tree, cols), f32),
    ]
    scratch = [s and pltpu.VMEM(*s) for s in vmem_scratch]
    scratch[4] = pltpu.SMEM((n, 8, HD), jnp.int32)
    sems = [
        dma((n,)),
        dma((n,)),
        dma((2, items)),
        dma((items,)),
        dma((items,)),
        dma((items,)),
        dma((items,)),
        dma((items,)),
        dma((items,)),
        dma((items,)),
        dma((items,)),
        dma((items + chunks,)),
        dma((items,)),
        dma((items + chunks,)),
        dma((1 + chunks + 2 * KVH,)),
    ]
    return pl.pallas_call(
        functools.partial(chain, n, cap, chunks, orders),
        out_shape=(
            jax.ShapeDtypeStruct((reqs, tree, width), bf16),
            jax.ShapeDtypeStruct((pages_here, HD), jnp.int32),
        ),
        in_specs=[smem] * 3 + [vmem] * 3 + [hbm] * 3,
        out_specs=(vmem, vmem),
        scratch_shapes=scratch + sems,
        compiler_params=pltpu.CompilerParams(
            collective_id=0, has_side_effects=True, vmem_limit_bytes=GRANT
        ),
        name="chain",
    )(
        page_table,
        prefix_lengths,
        live_lengths,
        tree_parents,
        tree_keys,
        tree_values,
        queries,
        page_keys,
        page_values,
    )


def attend(query_of, keys_of, values_of, allowed, out_to, stats, lane, first):
    for k in range(KVH):
        query = jnp.concatenate([query_of(k * GROUPS + g) for g in range(GROUPS)], axis=0)
        scores = (
            lax.dot_general(query, keys_of(k), NT, preferred_element_type=jnp.float32) * SCALE
        )
        scores = jnp.where(allowed, scores, NEG_BIG)
        peak = jnp.max(scores, axis=-1, keepdims=True)
        expo = jnp.exp(scores - peak)
        total = jnp.sum(expo, axis=-1, keepdims=True)
        out = jnp.dot(
            expo.astype(jnp.bfloat16), values_of(k), preferred_element_type=jnp.float32
        )
        rows = out.shape[0] // GROUPS
        for g in range(GROUPS):
            h = k * GROUPS + g
            part = slice(g * rows, (g + 1) * rows)
            out_to(h, out[part])
            stats = jnp.where(lane == first + h, peak[part], stats)
            stats = jnp.where(lane == first + QH + h, total[part], stats)
    return stats


def exchange(
    n,
    cap,
    table,
    prefix,
    live,
    parents_ref,
    q_ref,
    tk_ref,
    tv_ref,
    pk_hbm,
    pv_hbm,
    attended,
    reads_ref,
    pk_ref,
    pv_ref,
    target,
    used,
    label_ref,
    labels,
    label_now,
    got_out,
    got_stats,
    tree_out,
    tree_stats,
    q_all,
    q_now,
    out_send,
    stats_send,
    label_send_sem,
    label_recv_sem,
    q_send_sem,
    q_recv_sem,
    out_send_sem,
    out_recv_sem,
    stats_send_sem,
    stats_recv_sem,
    local_sem,
):
    reqs, tree, _ = q_ref.shape
    pages_here, page, _ = pk_ref.shape
    slots = table.shape[1]
    lanes = cap * 2 * QH
    fold = HD // lanes
    rows_held = tree // fold
    depth = n // 2
    me = lax.axis_index("pages")
    z, y = me // 2, me % 2
    other = 1 - y
    partner = z * 2 + other

    load_keys = pltpu.make_async_copy(pk_hbm, pk_ref, local_sem.at[2])
    load_values = pltpu.make_async_copy(pv_hbm, pv_ref, local_sem.at[3])
    load_keys.start()
    load_values.start()

    barrier = pltpu.get_barrier_semaphore()

    def greet(i, _):
        pl.semaphore_signal(
            barrier, inc=1, device_id={"pages": (me + i) % n}, device_id_type=MESH
        )
        return 0

    lax.fori_loop(1, n, greet, 0)
    pl.semaphore_wait(barrier, n - 1)

    def q_copy(src_ref, src, i, way, to):
        return pltpu.make_async_remote_copy(
            src_ref=src_ref,
            dst_ref=q_all.at[src, i],
            send_sem=q_send_sem.at[way, src // 2, i],
            recv_sem=q_recv_sem.at[src, i],
            device_id={"pages": to},
            device_id_type=MESH,
        )

    def out_copy(d):
        return pltpu.make_async_remote_copy(
            src_ref=out_send.at[d],
            dst_ref=got_out.at[pl.ds(me * cap, cap)],
            send_sem=out_send_sem.at[d],
            recv_sem=out_recv_sem.at[me],
            device_id={"pages": d},
            device_id_type=MESH,
        )

    def stats_copy(d):
        return pltpu.make_async_remote_copy(
            src_ref=stats_send.at[d],
            dst_ref=got_stats.at[me],
            send_sem=stats_send_sem.at[d],
            recv_sem=stats_recv_sem.at[me],
            device_id={"pages": d},
            device_id_type=MESH,
        )

    def q_arrive(src, i):
        pltpu.make_async_remote_copy(
            src_ref=q_all.at[src, i],
            dst_ref=q_all.at[src, i],
            send_sem=q_send_sem.at[0, src // 2, i],
            recv_sem=q_recv_sem.at[src, i],
            device_id={"pages": partner},
            device_id_type=MESH,
        ).wait_recv()

    for i in range(reqs):
        q_copy(q_ref.at[i], me, i, 2, partner).start()

        @pl.when(z + 1 < depth)
        def _():
            q_copy(q_ref.at[i], me, i, 0, me + 2).start()

        @pl.when(z > 0)
        def _():
            q_copy(q_ref.at[i], me, i, 1, me - 2).start()

    label_row = lax.broadcasted_iota(jnp.int32, (n, HD), 0)
    label_lane = lax.broadcasted_iota(jnp.int32, (n, HD), 1)
    told = jnp.zeros((n, HD), jnp.int32)
    owners, taken = [], []
    for p in range(reqs * slots):
        r, j = p // slots, p % slots
        count = jnp.clip(prefix[r] - j * page, 0, page)
        owner = lax.div(table[r, j], jnp.int32(pages_here))
        rank = jnp.int32(0)
        for earlier in range(p):
            same = (owners[earlier] == owner) & (taken[earlier] > 0)
            rank = rank + jnp.where(same, 1, 0)
        takes = jnp.where(count > 0, 1, 0)
        owners.append(owner)
        taken.append(takes)
        used[p] = takes
        target[p] = jnp.where(count > 0, owner * cap + rank, me * cap)
        row = label_row == jnp.where(count > 0, owner, -1)
        facts = (table[r, j] - owner * pages_here, count, r, live[r])
        for f, fact in enumerate(facts):
            told = jnp.where(row & (label_lane == rank * 4 + f), fact, told)
    for d in range(n):
        label_ref[d, 0:1, :] = told[d : d + 1]

    def label_copy(d):
        return pltpu.make_async_remote_copy(
            src_ref=label_ref.at[d],
            dst_ref=labels.at[me],
            send_sem=label_send_sem.at[d],
            recv_sem=label_recv_sem.at[me],
            device_id={"pages": d},
            device_id_type=MESH,
        )

    def tell(i, _):
        label_copy((me + i) % n).start()
        return 0

    lax.fori_loop(1, n, tell, 0)

    lane = lax.broadcasted_iota(jnp.int32, (tree, HD), 1)
    key_lane = lax.broadcasted_iota(jnp.int32, (GROUPS * tree, page), 1)

    def serve(d):
        stats = jnp.zeros((tree, HD), jnp.float32)
        for c in range(cap):
            which, count, req = (label_now[d, 0, c * 4 + f] for f in range(3))

            def out_to(h, value):
                out_send[d, c, :, head(h)] = value.astype(jnp.bfloat16)

            stats = attend(
                lambda h: q_now[req, :, head(h)],
                lambda k: pk_ref[which, :, head(k)],
                lambda k: pv_ref[which, :, head(k)],
                key_lane < count,
                out_to,
                stats,
                lane,
                c * 2 * QH,
            )
        stats_send[d] = jnp.concatenate(
            [stats[i * rows_held : (i + 1) * rows_held, :lanes] for i in range(fold)], axis=1
        )

    def one_tree(r, _):
        source = lax.broadcasted_iota(jnp.int32, (tree, tree), 0)
        child = lax.broadcasted_iota(jnp.int32, (tree, tree), 1)
        linked = (source == parents_ref[pl.ds(r, 1), :]) | (source == child)
        same = jnp.where(source == child, 1.0, 0.0).astype(jnp.bfloat16)
        reach = jnp.where(linked, 1.0, 0.0).astype(jnp.bfloat16)
        for level in range((tree - 1).bit_length()):
            reach = jnp.where(
                jnp.dot(reach, reach, preferred_element_type=jnp.float32) > 0, 1.0, 0.0
            ).astype(jnp.bfloat16)
        upright = lax.dot_general(
            reach, same, (((0,), (0,)), ((), ())), preferred_element_type=jnp.float32
        )
        open_ = jnp.where(child < live[r], upright, 0.0)
        allowed = jnp.concatenate([open_] * GROUPS, axis=0) > 0

        def out_to(h, value):
            tree_out[r, :, head(h)] = value

        tree_stats[r] = attend(
            lambda h: q_ref[r, :, head(h)],
            lambda k: tk_ref[r, :, head(k)],
            lambda k: tv_ref[r, :, head(k)],
            allowed,
            out_to,
            jnp.zeros((tree, HD), jnp.float32),
            lane,
            0,
        )
        return 0

    lax.fori_loop(0, reqs, one_tree, 0)

    labels[me] = label_ref[me]

    def hear(i, _):
        d = (me + i) % n
        pltpu.make_async_remote_copy(
            src_ref=label_ref.at[d],
            dst_ref=labels.at[d],
            send_sem=label_send_sem.at[d],
            recv_sem=label_recv_sem.at[d],
            device_id={"pages": d},
            device_id_type=MESH,
        ).wait()
        return 0

    lax.fori_loop(1, n, hear, 0)
    into_scalars = pltpu.make_async_copy(labels, label_now, local_sem.at[0])
    into_scalars.start()
    into_scalars.wait()
    load_keys.wait()
    load_values.wait()

    q_now[...] = q_ref[...]
    serve(me)
    for c in range(cap):
        got_out[me * cap + c] = out_send[me, c]
    got_stats[me] = stats_send[me]

    page_row = lax.broadcasted_iota(jnp.int32, (pages_here, HD), 0)

    def count_reads(d, reads):
        for c in range(cap):
            which, count, _, lives = (label_now[d, 0, c * 4 + f] for f in range(4))
            lives = jnp.where(count > 0, lives, 0)
            reads = reads + jnp.where(page_row == which, lives, 0)
        return reads

    reads_ref[...] = lax.fori_loop(
        0, n, count_reads, jnp.zeros((pages_here, HD), jnp.int32)
    )

    def step(s, _):
        for i in range(reqs):

            @pl.when(z - s >= 0)
            def _():
                src = me - 2 * s
                q_arrive(src, i)
                q_copy(q_all.at[src, i], src, i, 2, partner).start()

                @pl.when(z + 1 < depth)
                def _():
                    q_copy(q_all.at[src, i], src, i, 0, me + 2).start()

            @pl.when(z + s < depth)
            def _():
                src = me + 2 * s
                q_arrive(src, i)
                q_copy(q_all.at[src, i], src, i, 2, partner).start()

                @pl.when(z > 0)
                def _():
                    q_copy(q_all.at[src, i], src, i, 1, me - 2).start()

        def case(k, _):
            crossed = k // 2
            far = s - crossed
            row = z + far * (2 * (k % 2) - 1)
            column = y + crossed * (other - y)
            d = row * 2 + column
            valid = (row >= 0) & (row < depth) & ((far > 0) | (k == 2))

            @pl.when(valid)
            def _():
                @pl.when(crossed == 1)
                def _():
                    for i in range(reqs):
                        q_arrive(d, i)

                q_now[...] = q_all[d]
                serve(d)
                out_copy(d).start()
                stats_copy(d).start()

            return 0

        lax.fori_loop(0, 4, case, 0)
        return 0

    lax.fori_loop(1, depth + 1, step, 0)

    def finish(i, _):
        d = (me + i) % n
        out_copy(d).wait_send()
        stats_copy(d).wait_send()
        pltpu.make_async_remote_copy(
            src_ref=out_send.at[d],
            dst_ref=got_out.at[pl.ds(d * cap, cap)],
            send_sem=out_send_sem.at[d],
            recv_sem=out_recv_sem.at[d],
            device_id={"pages": d},
            device_id_type=MESH,
        ).wait_recv()
        pltpu.make_async_remote_copy(
            src_ref=stats_send.at[d],
            dst_ref=got_stats.at[d],
            send_sem=stats_send_sem.at[d],
            recv_sem=stats_recv_sem.at[d],
            device_id={"pages": d},
            device_id_type=MESH,
        ).wait_recv()
        return 0

    lax.fori_loop(1, n, finish, 0)

    def drain(row, _):
        src = row * 2 + y
        for i in range(reqs):
            q_copy(q_all.at[src, i], src, i, 2, partner).wait_send()

            @pl.when((row <= z) & (z + 1 < depth))
            def _():
                q_copy(q_all.at[src, i], src, i, 0, me + 2).wait_send()

            @pl.when((row >= z) & (z > 0))
            def _():
                q_copy(q_all.at[src, i], src, i, 1, me - 2).wait_send()

        return 0

    lax.fori_loop(0, depth, drain, 0)

    def merge(r, _):
        tree_peak, tree_total = tree_stats[r, :, :QH], tree_stats[r, :, QH : 2 * QH]
        top = tree_peak
        peaks, totals = [], []
        for j in range(slots):
            where_ = target[r * slots + j]
            live_slot = used[r * slots + j] > 0
            packed = got_stats[where_ // cap]
            held = jnp.concatenate(
                [packed[:, i * lanes : (i + 1) * lanes] for i in range(fold)], axis=0
            )
            mine = held[:, : 2 * QH]
            for c in range(1, cap):
                mine = jnp.where(
                    where_ % cap == c, held[:, c * 2 * QH : (c + 1) * 2 * QH], mine
                )
            peaks.append(jnp.where(live_slot, mine[:, :QH], NEG_BIG))
            totals.append(mine[:, QH:])
            top = jnp.maximum(top, peaks[j])
        tree_scale = jnp.exp(tree_peak - top)
        scales = [
            jnp.where(used[r * slots + j] > 0, jnp.exp(peaks[j] - top), 0.0)
            for j in range(slots)
        ]
        total = tree_total * tree_scale
        for j in range(slots):
            total = total + scales[j] * totals[j]
        tree_scale = tree_scale / total
        scales = [scale / total for scale in scales]
        for h in range(QH):
            mixed = tree_out[r, :, head(h)] * tree_scale[:, h : h + 1]
            for j in range(slots):
                part = got_out[target[r * slots + j], :, head(h)].astype(jnp.float32)
                mixed = mixed + part * scales[j][:, h : h + 1]
            attended[r, :, head(h)] = mixed.astype(jnp.bfloat16)
        return 0

    lax.fori_loop(0, reqs, merge, 0)


def shards(
    queries,
    tree_keys,
    tree_values,
    page_keys,
    page_values,
    page_table,
    prefix_lengths,
    tree_parents,
    live_lengths,
):
    n = lax.axis_size("pages")
    reqs, tree, width = queries.shape
    pages_here = page_keys.shape[0]
    slots = page_table.shape[1]
    pairs = reqs * slots
    cap = max(1, pairs // n)
    args = (queries, tree_keys, tree_values, page_keys, page_values)
    args += (page_table, prefix_lengths, tree_parents, live_lengths)
    if 7 * n * reqs * tree * width < GRANT:
        attended, reads = chain_call(n, cap, args)
        return attended, reads[:, 0]

    smem = pl.BlockSpec(memory_space=pltpu.SMEM)
    vmem = pl.BlockSpec(memory_space=pltpu.VMEM)
    hbm = pl.BlockSpec(memory_space=pl.ANY)
    depth = n // 2
    held_stats = (n, tree * cap * 2 * QH // HD, HD)
    attended, reads = pl.pallas_call(
        functools.partial(exchange, n, cap),
        out_shape=(
            jax.ShapeDtypeStruct((reqs, tree, width), jnp.bfloat16),
            jax.ShapeDtypeStruct((pages_here, HD), jnp.int32),
        ),
        in_specs=[smem] * 3 + [vmem] * 4 + [hbm] * 2,
        out_specs=(vmem, vmem),
        scratch_shapes=[
            pltpu.VMEM(page_keys.shape, jnp.bfloat16),
            pltpu.VMEM(page_values.shape, jnp.bfloat16),
            pltpu.SMEM((pairs,), jnp.int32),
            pltpu.SMEM((pairs,), jnp.int32),
            pltpu.VMEM((n, 8, HD), jnp.int32),
            pltpu.VMEM((n, 8, HD), jnp.int32),
            pltpu.SMEM((n, 8, HD), jnp.int32),
            pltpu.VMEM((n * cap, tree, width), jnp.bfloat16),
            pltpu.VMEM(held_stats, jnp.float32),
            pltpu.VMEM((reqs, tree, width), jnp.float32),
            pltpu.VMEM((reqs, tree, HD), jnp.float32),
            pltpu.VMEM((n, reqs, tree, width), jnp.bfloat16),
            pltpu.VMEM((reqs, tree, width), jnp.bfloat16),
            pltpu.VMEM((n, cap, tree, width), jnp.bfloat16),
            pltpu.VMEM(held_stats, jnp.float32),
            pltpu.SemaphoreType.DMA((n,)),
            pltpu.SemaphoreType.DMA((n,)),
            pltpu.SemaphoreType.DMA((3, depth, reqs)),
            pltpu.SemaphoreType.DMA((n, reqs)),
            pltpu.SemaphoreType.DMA((n,)),
            pltpu.SemaphoreType.DMA((n,)),
            pltpu.SemaphoreType.DMA((n,)),
            pltpu.SemaphoreType.DMA((n,)),
            pltpu.SemaphoreType.DMA((4,)),
        ],
        compiler_params=pltpu.CompilerParams(
            collective_id=0, has_side_effects=True, vmem_limit_bytes=63 * 1024 * 1024
        ),
        name="exchange",
    )(
        page_table,
        prefix_lengths,
        live_lengths,
        tree_parents,
        queries,
        tree_keys,
        tree_values,
        page_keys,
        page_values,
    )
    return (attended, reads[:, 0])


def solution(mesh):
    rows = P(("grp", "pages"), None, None)
    return jax.shard_map(
        shards,
        mesh=mesh,
        in_specs=(
            rows,
            rows,
            rows,
            rows,
            rows,
            P(("grp", "pages"), None),
            P(("grp", "pages")),
            P(("grp", "pages"), None),
            P(("grp", "pages")),
        ),
        out_specs=(rows, P(("grp", "pages"))),
        check_vma=False,
    )
```

```python
import functools
import heapq
import itertools

import jax
import jax.numpy as jnp
from jax import lax
from jax.experimental import pallas as pl
from jax.experimental.pallas import tpu as pltpu
from jax.sharding import PartitionSpec as P

QH = 16
KVH = 4
HD = 128
GROUPS = QH // KVH
NEG_BIG = -1e30
SCALE = HD ** (-0.5)
LOG2E = 1.4426950408889634
NT = (((1,), (1,)), ((), ()))
TN = (((0,), (0,)), ((), ()))
MESH = pl.DeviceIdType.MESH
CHUNKS = 4
EARLY = 2
EARLY_Y = 2
GRANT = 63 * 1024 * 1024

PICK, LOCAL, ACROSS, MERGE, Q_RIGHT, Q_LEFT, STATE, Y_QUERY, Y_PART = range(9)


def split(value, size):
    if size & (size - 1):
        return value // size, value % size
    return value >> (size.bit_length() - 1), value & (size - 1)


def head(h):
    return slice(h * HD, (h + 1) * HD)


WEIGHTS = ((40, 20, 0.5), (100, 15, 0.0), (20, 5, 5.0), (40, 20, 3.0))


def plan(depth, chunks, start=5.0, own=0.8, delay=2.6, weights=WEIGHTS):
    per = 4.0 / chunks
    wire = {Q_RIGHT: 5.63 * per, Q_LEFT: 5.63 * per, STATE: 5.8 * per}
    wire.update({Y_QUERY: 2.82 * per, Y_PART: 2.9 * per})
    work = {PICK: 0.2, LOCAL: 0.45, ACROSS: 0.45, MERGE: 0.5}
    rank = {PICK: 0, ACROSS: 1, MERGE: 2, LOCAL: 3}
    events, tick = [], itertools.count()
    have = [set() for _ in range(depth)]
    queue, busy, last = {}, {}, {}
    idle = [False] * depth
    todo = [
        {
            (kind, s, k)
            for kind in rank
            for s in range(depth)
            for k in range(chunks)
            if kind != PICK or s != z
        }
        for z in range(depth)
    ]
    issued = [[] for _ in range(depth)]

    def post(time, what, *facts):
        heapq.heappush(events, (time, next(tick), what, facts))

    def pump(time, key):
        if busy.get(key) or not queue.get(key):
            return
        _, _, ready, op, tag, dest = heapq.heappop(queue[key])
        busy[key] = True
        issued[key[0]].append((max(ready, last.get(key, 0.0)), 0, next(tick), op))
        last[key] = time
        post(time + wire[op[0]], "free", key)
        post(time + wire[op[0]] + delay, "land", tag, dest)

    def send(time, z, link, op, tag, dest):
        late = op[0] not in (Q_RIGHT, Q_LEFT, Y_QUERY)
        a, b, c = weights[2 * (link == "y") + late]
        order = a - b * abs(op[1] - z) + c * op[2]
        heapq.heappush(
            queue.setdefault((z, link), []), (order, next(tick), time, op, tag, dest)
        )
        pump(time, (z, link))

    def send_query(time, z, s, k):
        if s <= z < depth - 1:
            send(time, z, "right", (Q_RIGHT, s, k), ("q", s, k), z + 1)
        if s >= z > 0:
            send(time, z, "left", (Q_LEFT, s, k), ("q", s, k), z - 1)

    def ready(z, op):
        kind, s, k = op
        if kind == PICK:
            return s == z or ("q", s, k) in have[z]
        if kind == LOCAL:
            return s == z or (PICK, s, k) in have[z]
        if kind == ACROSS:
            return ("yq", s, k) in have[z]
        need = [(LOCAL, s, k), ("yp", s, k)]
        need += [("right", s, k)] * (s >= z and z > 0)
        need += [("left", s, k)] * (s <= z and z < depth - 1)
        return all(n in have[z] for n in need)

    def turn(time, z):
        if not idle[z]:
            return
        able = [op for op in todo[z] if ready(z, op)]
        if not able:
            return
        op = min(able, key=lambda o: (rank[o[0]], -abs(o[1] - z), o[2], o[1]))
        todo[z].remove(op)
        issued[z].append((time, 1, next(tick), op))
        idle[z] = False
        if op[0] == PICK:
            send_query(time + 1e-3, z, op[1], op[2])
        post(time + work[op[0]], "done", z, op)

    for z in range(depth):
        for k in range(chunks):
            send_query(0.0, z, z, k)
            post(own, "pick", z, k)
        post(start, "done", z, None)
    while events:
        time, _, what, facts = heapq.heappop(events)
        if what == "free":
            busy[facts[0]] = False
            pump(time, facts[0])
        elif what == "pick":
            z, k = facts
            send(time, z, "y", (Y_QUERY, z, k), ("yq", z, k), z)
        elif what == "land":
            have[facts[1]].add(facts[0])
            turn(time, facts[1])
        else:
            z, op = facts
            idle[z] = True
            if op is not None:
                kind, s, k = op
                have[z].add(op)
                if kind == PICK:
                    send(time, z, "y", (Y_QUERY, s, k), ("yq", s, k), z)
                elif kind == ACROSS:
                    send(time, z, "y", (Y_PART, s, k), ("yp", s, k), z)
                elif kind == MERGE and s > z:
                    send(time, z, "right", (STATE, s, k), ("right", s, k), z + 1)
                elif kind == MERGE and s < z:
                    send(time, z, "left", (STATE, s, k), ("left", s, k), z - 1)
            turn(time, z)
    items = depth * chunks
    early, early_y = EARLY, EARLY_Y
    orders = [
        [
            op[0] * items + op[1] * chunks + op[2]
            for _, _, _, op in sorted(steps)
            if not (op[0] in (Q_RIGHT, Q_LEFT) and op[1] == z and op[2] < early)
            and not (op[0] == Y_QUERY and op[1] == z and op[2] < early_y)
        ]
        for z, steps in enumerate(issued)
    ]
    longest = max(len(o) for o in orders)
    return [o + [-1] * (longest - len(o)) for o in orders]


def attend_parts(queries, keys, values, allowed):
    scores = [
        lax.dot_general(k, q, NT, preferred_element_type=jnp.float32)
        for q, k in zip(queries, keys)
    ]
    scores = [jnp.where(a, s, NEG_BIG) for s, a in zip(scores, allowed)]
    peaks = [jnp.max(s, axis=0, keepdims=True) for s in scores]
    expos = [jnp.exp2((s - p) * (SCALE * LOG2E)) for s, p in zip(scores, peaks)]
    totals = [jnp.sum(e, axis=0, keepdims=True) for e in expos]
    outs = [
        lax.dot_general(
            v, e.astype(jnp.bfloat16), TN, preferred_element_type=jnp.float32
        )
        for v, e in zip(values, expos)
    ]
    outs = [o * (1.0 / t) for o, t in zip(outs, totals)]
    return outs, [p * SCALE + jnp.log(t) for p, t in zip(peaks, totals)]


def chain(
    n,
    cap,
    chunks,
    orders,
    table,
    prefix,
    live,
    parents_ref,
    tk_ref,
    tv_ref,
    q_hbm,
    pk_hbm,
    pv_hbm,
    attended,
    reads_ref,
    pk_ref,
    pv_ref,
    label_ref,
    labels,
    label_now,
    qa,
    q_now,
    yq_send,
    yq_got,
    yo_send,
    yo_got,
    ys_send,
    ys_got,
    loc_o,
    loc_s,
    st_o,
    st_s,
    tree_o,
    tree_s,
    open_ref,
    label_send_sem,
    label_recv_sem,
    q_send_sem,
    q_recv_sem,
    yq_send_sem,
    yq_recv_sem,
    yo_send_sem,
    yo_recv_sem,
    ys_send_sem,
    ys_recv_sem,
    so_send_sem,
    so_recv_sem,
    ss_send_sem,
    ss_recv_sem,
    local_sem,
):
    reqs, tree, wide = q_now.shape
    _, pages_here, page, _ = pk_ref.shape
    slots = table.shape[1]
    depth = n // 2
    items = depth * chunks
    heads = wide // HD
    cols = heads * tree
    tiles = cols // HD
    me = lax.axis_index("pages")
    z, y = me // 2, me % 2
    partner = z * 2 + (1 - y)
    absent = items + chunks

    loads = []
    for k in range(chunks):
        loads.append(
            pltpu.make_async_copy(
                q_hbm.at[:, :, pl.ds(k * wide, wide)],
                qa.at[z * chunks + k],
                local_sem.at[1 + k],
            )
        )
    page_loads = []
    for k in range(KVH):
        for f, (src, dst) in enumerate(((pk_hbm, pk_ref), (pv_hbm, pv_ref))):
            page_loads.append(
                pltpu.make_async_copy(
                    src.at[:, :, pl.ds(k * HD, HD)],
                    dst.at[k],
                    local_sem.at[1 + chunks + 2 * k + f],
                )
            )
    for copy in loads + page_loads:
        copy.start()

    barrier = pltpu.get_barrier_semaphore()

    def greet(i, _):
        pl.semaphore_signal(
            barrier, inc=1, device_id={"pages": (me + i) % n}, device_id_type=MESH
        )
        return 0

    lax.fori_loop(1, n, greet, 0)

    label_row = lax.broadcasted_iota(jnp.int32, (n, HD), 0)
    label_lane = lax.broadcasted_iota(jnp.int32, (n, HD), 1)
    told = jnp.zeros((n, HD), jnp.int32)
    owners, taken = [], []
    asked = [jnp.int32(0)] * cap
    for p in range(reqs * slots):
        r, j = p // slots, p % slots
        count = jnp.clip(prefix[r] - j * page, 0, page)
        owner = lax.div(table[r, j], jnp.int32(pages_here))
        rank = jnp.int32(0)
        for earlier in range(p):
            same = (owners[earlier] == owner) & (taken[earlier] > 0)
            rank = rank + jnp.where(same, 1, 0)
        owners.append(owner)
        taken.append(jnp.where(count > 0, 1, 0))
        beside = (owner == partner) & (count > 0)
        asked = [jnp.where(beside & (rank == c), r, a) for c, a in enumerate(asked)]
        row = label_row == jnp.where(count > 0, owner, -1)
        facts = (table[r, j] - owner * pages_here, count, r, live[r])
        for f, fact in enumerate(facts):
            told = jnp.where(row & (label_lane == rank * 4 + f), fact, told)
    for d in range(depth):
        label_ref[d, 0:2, :] = told[2 * d : 2 * d + 2]

    def q_copy(j, way):
        return pltpu.make_async_remote_copy(
            src_ref=qa.at[j],
            dst_ref=qa.at[j],
            send_sem=q_send_sem.at[way, j],
            recv_sem=q_recv_sem.at[j],
            device_id={"pages": me + 2 - 4 * way},
            device_id_type=MESH,
        )

    def across(src, dst, send_sem, recv_sem, j):
        return pltpu.make_async_remote_copy(
            src_ref=src.at[j],
            dst_ref=dst.at[j],
            send_sem=send_sem.at[j],
            recv_sem=recv_sem.at[j],
            device_id={"pages": partner},
            device_id_type=MESH,
        )

    def yq_copy(j):
        return across(yq_send, yq_got, yq_send_sem, yq_recv_sem, j)

    def yo_copy(j):
        return across(yo_send, yo_got, yo_send_sem, yo_recv_sem, j)

    def ys_copy(j):
        return across(ys_send, ys_got, ys_send_sem, ys_recv_sem, j)

    def state_copies(j, row, k):
        left = jnp.where(row < z, 1, 0)
        ends = left * jnp.where(row == z - 1, 1, 0)
        slot = j + ends * (items - row * chunks)
        to = {"pages": me + 2 - 4 * left}
        return (
            pltpu.make_async_remote_copy(
                src_ref=st_o.at[j],
                dst_ref=st_o.at[slot],
                send_sem=so_send_sem.at[j],
                recv_sem=so_recv_sem.at[slot],
                device_id=to,
                device_id_type=MESH,
            ),
            pltpu.make_async_remote_copy(
                src_ref=st_s.at[j],
                dst_ref=st_s.at[slot],
                send_sem=ss_send_sem.at[j],
                recv_sem=ss_recv_sem.at[slot],
                device_id=to,
                device_id_type=MESH,
            ),
        )

    def state_arrive(slot):
        for ref, sem in ((st_o, so_recv_sem), (st_s, ss_recv_sem)):
            pltpu.make_async_remote_copy(
                src_ref=ref.at[slot],
                dst_ref=ref.at[slot],
                send_sem=sem.at[slot],
                recv_sem=sem.at[slot],
                device_id={"pages": partner},
                device_id_type=MESH,
            ).wait_recv()

    pl.semaphore_wait(barrier, n - 1)

    def label_copy(d):
        return pltpu.make_async_remote_copy(
            src_ref=label_ref.at[d // 2],
            dst_ref=labels.at[me],
            send_sem=label_send_sem.at[d],
            recv_sem=label_recv_sem.at[me],
            device_id={"pages": d},
            device_id_type=MESH,
        )

    def tell(i, _):
        label_copy((me + i) % n).start()
        return 0

    lax.fori_loop(1, n, tell, 0)

    for copy in loads:
        copy.wait()

    for k in range(EARLY):
        j = z * chunks + k

        @pl.when(z < depth - 1)
        def _():
            q_copy(j, 0).start()

        @pl.when(z > 0)
        def _():
            q_copy(j, 1).start()

    def own_pick(k, _):
        j = z * chunks + k
        q_now[...] = qa[j]
        for c in range(cap):
            yq_send[j, c] = q_now[asked[c]]

        @pl.when(k < EARLY_Y)
        def _():
            yq_copy(j).start()

        return 0

    lax.fori_loop(0, chunks, own_pick, 0)

    bits = (9 * items).bit_length()
    per_word = 31 // bits
    steps = -(-len(orders[0]) // per_word)
    words = []
    for w in range(steps):
        packed = []
        for o in orders:
            few = o[w * per_word : (w + 1) * per_word]
            few = few + [-1] * (per_word - len(few))
            packed.append(
                sum((9 * items if c < 0 else c) << (bits * b) for b, c in enumerate(few))
            )
        word = jnp.int32(packed[0])
        for row in range(1, depth):
            if packed[row] != packed[0]:
                word = jnp.where(z == row, packed[row], word)
        words.append(word)

    st_o[absent] = jnp.zeros_like(st_o[absent])
    st_s[absent] = jnp.full(st_s.shape[1:], NEG_BIG, jnp.float32)

    def rows_of(query):
        return jnp.concatenate([query[:, head(h)] for h in range(heads)], axis=0)

    def put_row(ref, index, first, vector):
        for i in range(tiles):
            ref[index, first + i : first + i + 1, :] = vector[:, head(i)]

    def get_row(tile, first):
        return jnp.concatenate(
            [tile[first + i : first + i + 1, :] for i in range(tiles)], axis=1
        )

    source = lax.broadcasted_iota(jnp.int32, (tree, tree), 0)
    child = lax.broadcasted_iota(jnp.int32, (tree, tree), 1)
    reaches = []
    for r in range(reqs):
        linked = (source == parents_ref[r : r + 1, :]) | (source == child)
        reaches.append(jnp.where(linked, 1.0, 0.0).astype(jnp.bfloat16))
    for level in range((tree - 1).bit_length()):
        reaches = [
            jnp.where(
                jnp.dot(reach, reach, preferred_element_type=jnp.float32) > 0, 1.0, 0.0
            ).astype(jnp.bfloat16)
            for reach in reaches
        ]
    for r in range(reqs):
        open_ = jnp.where(source < live[r], reaches[r].astype(jnp.float32), 0.0)
        open_ref[r] = jnp.concatenate([open_] * heads, axis=1)

    def tree_step(k, _):
        kv = k * heads // GROUPS
        lanes = pl.ds(pl.multiple_of(kv * HD, HD), HD)
        every = range(reqs)
        outs, lses = attend_parts(
            [rows_of(qa[z * chunks + k, r]) for r in every],
            [tk_ref[r, :, lanes] for r in every],
            [tv_ref[r, :, lanes] for r in every],
            [open_ref[r] > 0 for r in every],
        )
        for r in every:
            tree_o[k, r] = outs[r]
            put_row(tree_s, k, r * tiles, lses[r])
        return 0

    lax.fori_loop(0, chunks, tree_step, 0)

    labels[me] = label_ref[z]

    def hear(i, _):
        d = (me + i) % n
        pltpu.make_async_remote_copy(
            src_ref=label_ref.at[d // 2],
            dst_ref=labels.at[d],
            send_sem=label_send_sem.at[d],
            recv_sem=label_recv_sem.at[d],
            device_id={"pages": d},
            device_id_type=MESH,
        ).wait()
        return 0

    lax.fori_loop(1, n, hear, 0)
    into_scalars = pltpu.make_async_copy(labels, label_now, local_sem.at[0])
    into_scalars.start()
    into_scalars.wait()
    for copy in page_loads:
        copy.wait()

    key_row = lax.broadcasted_iota(jnp.int32, (page, cols), 0)

    def serve(d, k, query_of, out_ref, stat_ref, j):
        kv = k * heads // GROUPS
        facts = [[label_now[d, y, c * 4 + f] for f in range(3)] for c in range(cap)]
        outs, lses = attend_parts(
            [rows_of(query_of(c, req)) for c, (_, _, req) in enumerate(facts)],
            [pk_ref[kv, which] for which, _, _ in facts],
            [pv_ref[kv, which] for which, _, _ in facts],
            [key_row < count for _, count, _ in facts],
        )
        for c in range(cap):
            out_ref[j, c] = outs[c].astype(jnp.bfloat16)
            put_row(stat_ref, j, c * tiles, lses[c])

    def pick(j, row, k):
        pltpu.make_async_remote_copy(
            src_ref=qa.at[j],
            dst_ref=qa.at[j],
            send_sem=q_send_sem.at[0, j],
            recv_sem=q_recv_sem.at[j],
            device_id={"pages": partner},
            device_id_type=MESH,
        ).wait_recv()
        q_now[...] = qa[j]
        for c in range(cap):
            yq_send[j, c] = q_now[label_now[row * 2 + y, 1 - y, c * 4 + 2]]

    def local(j, row, k):
        q_now[...] = qa[j]
        serve(row * 2 + y, k, lambda c, req: q_now[req], loc_o, loc_s, j)

    def from_partner(j, row, k):
        yq_copy(j).wait_recv()
        serve(row * 2 + (1 - y), k, lambda c, req: yq_got[j, c], yo_send, ys_send, j)

    def merged(j, row, r, others):
        parts, weights = [], []
        for held_o, held_s, owner in ((loc_o, loc_s, y), (yo_got, ys_got, 1 - y)):
            tile = held_s[j]
            for c in range(cap):
                count, req = (label_now[row * 2 + y, owner, c * 4 + f] for f in (1, 2))
                mine = (count > 0) & (req == r)
                parts.append(held_o[j, c].astype(jnp.float32))
                weights.append(jnp.where(mine, get_row(tile, c * tiles), NEG_BIG))
        for part, lse in others:
            parts.append(part)
            weights.append(lse)
        top = functools.reduce(jnp.maximum, weights)
        weights = [jnp.exp(w - top) for w in weights]
        total = functools.reduce(jnp.add, weights)
        rest = 1.0 / total
        out = parts[0] * (weights[0] * rest)
        for part, weight in zip(parts[1:], weights[1:]):
            out = out + part * (weight * rest)
        return out, top + jnp.log(total)

    def state_part(slot, r):
        return st_o[slot, r].astype(jnp.float32), get_row(st_s[slot], r * tiles)

    def merge(j, row, k):
        yo_copy(j).wait_recv()
        ys_copy(j).wait_recv()

        @pl.when(row != z)
        def _():
            comes = jnp.where(
                row > z, jnp.where(z > 0, 1, 0), jnp.where(z < depth - 1, 1, 0)
            )
            slot = absent + comes * (j - absent)

            @pl.when(comes == 1)
            def _():
                state_arrive(j)

            for r in range(reqs):
                out, lse = merged(j, row, r, [state_part(slot, r)])
                st_o[j, r] = out.astype(jnp.bfloat16)
                put_row(st_s, j, r * tiles, lse)

        @pl.when(row == z)
        def _():
            right = absent + jnp.where(z > 0, 1, 0) * (j - absent)
            left = absent + jnp.where(z < depth - 1, 1, 0) * (items + k - absent)

            @pl.when(z > 0)
            def _():
                state_arrive(j)

            @pl.when(z < depth - 1)
            def _():
                state_arrive(items + k)

            for r in range(reqs):
                own = tree_o[k, r], get_row(tree_s[k], r * tiles)
                out, _ = merged(
                    j, row, r, [state_part(right, r), state_part(left, r), own]
                )
                upright = out.T.astype(jnp.bfloat16)
                for h in range(heads):
                    lanes = pl.ds(pl.multiple_of(k * wide + h * HD, HD), HD)
                    attended[r, :, lanes] = upright[h * tree : (h + 1) * tree]

    def step(b, word):
        code = (word >> (bits * b)) & ((1 << bits) - 1)
        kind, j = split(code, items)
        row, k = split(j, chunks)

        @pl.when(kind < Q_RIGHT)
        def _():
            @pl.when(kind < ACROSS)
            def _():
                @pl.when(kind == PICK)
                def _():
                    pick(j, row, k)

                @pl.when(kind == LOCAL)
                def _():
                    local(j, row, k)

            @pl.when(kind >= ACROSS)
            def _():
                @pl.when(kind == ACROSS)
                def _():
                    from_partner(j, row, k)

                @pl.when(kind == MERGE)
                def _():
                    merge(j, row, k)

        @pl.when(kind >= Q_RIGHT)
        def _():
            @pl.when(kind < STATE)
            def _():
                @pl.when(kind == Q_RIGHT)
                def _():
                    q_copy(j, 0).start()

                @pl.when(kind == Q_LEFT)
                def _():
                    q_copy(j, 1).start()

            @pl.when(kind == STATE)
            def _():
                for copy in state_copies(j, row, k):
                    copy.start()

            @pl.when(kind == Y_QUERY)
            def _():
                yq_copy(j).start()

            @pl.when(kind == Y_PART)
            def _():
                yo_copy(j).start()
                ys_copy(j).start()

        return word

    def take(w, _):
        word = words[0]
        for i in range(1, steps):
            word = jnp.where(w == i, words[i], word)
        lax.fori_loop(0, per_word, step, word)
        return 0

    lax.fori_loop(0, steps, take, 0)

    page_row = lax.broadcasted_iota(jnp.int32, (pages_here, HD), 0)

    def count_reads(d, reads):
        for c in range(cap):
            which, count, _, lives = (label_now[d, y, c * 4 + f] for f in range(4))
            lives = jnp.where(count > 0, lives, 0)
            reads = reads + jnp.where(page_row == which, lives, 0)
        return reads

    reads_ref[...] = lax.fori_loop(
        0, n, count_reads, jnp.zeros((pages_here, HD), jnp.int32)
    )

    def drain(j, _):
        row, k = j // chunks, j % chunks
        yq_copy(j).wait_send()
        yo_copy(j).wait_send()
        ys_copy(j).wait_send()

        @pl.when((row <= z) & (z < depth - 1))
        def _():
            q_copy(j, 0).wait_send()

        @pl.when((row >= z) & (z > 0))
        def _():
            q_copy(j, 1).wait_send()

        @pl.when(row != z)
        def _():
            for copy in state_copies(j, row, k):
                copy.wait_send()

        return 0

    lax.fori_loop(0, items, drain, 0)


def chain_call(n, cap, args):
    queries, tree_keys, tree_values, page_keys, page_values = args[:5]
    page_table, prefix_lengths, tree_parents, live_lengths = args[5:]
    reqs, tree, width = queries.shape
    pages_here, page, _ = page_keys.shape
    chunks, depth = CHUNKS, n // 2
    items = depth * chunks
    wide = width // chunks
    cols = wide // HD * tree
    few, many = cap * cols // HD, reqs * cols // HD
    bf16, f32 = jnp.bfloat16, jnp.float32
    dma = pltpu.SemaphoreType.DMA
    smem = pl.BlockSpec(memory_space=pltpu.SMEM)
    vmem = pl.BlockSpec(memory_space=pltpu.VMEM)
    hbm = pl.BlockSpec(memory_space=pl.ANY)
    orders = plan(depth, chunks)
    vmem_scratch = [
        ((KVH, pages_here, page, HD), bf16),
        ((KVH, pages_here, page, HD), bf16),
        ((depth, 8, HD), jnp.int32),
        ((n, 8, HD), jnp.int32),
        None,
        ((items, reqs, tree, wide), bf16),
        ((reqs, tree, wide), bf16),
        ((items, cap, tree, wide), bf16),
        ((items, cap, tree, wide), bf16),
        ((items, cap, HD, cols), bf16),
        ((items, cap, HD, cols), bf16),
        ((items, few, HD), f32),
        ((items, few, HD), f32),
        ((items, cap, HD, cols), bf16),
        ((items, few, HD), f32),
        ((items + chunks + 1, reqs, HD, cols), bf16),
        ((items + chunks + 1, many, HD), f32),
        ((chunks, reqs, HD, cols), f32),
        ((chunks, many, HD), f32),
        ((reqs, tree, cols), f32),
    ]
    scratch = [s and pltpu.VMEM(*s) for s in vmem_scratch]
    scratch[4] = pltpu.SMEM((n, 8, HD), jnp.int32)
    sems = [
        dma((n,)),
        dma((n,)),
        dma((2, items)),
        dma((items,)),
        dma((items,)),
        dma((items,)),
        dma((items,)),
        dma((items,)),
        dma((items,)),
        dma((items,)),
        dma((items,)),
        dma((items + chunks,)),
        dma((items,)),
        dma((items + chunks,)),
        dma((1 + chunks + 2 * KVH,)),
    ]
    return pl.pallas_call(
        functools.partial(chain, n, cap, chunks, orders),
        out_shape=(
            jax.ShapeDtypeStruct((reqs, tree, width), bf16),
            jax.ShapeDtypeStruct((pages_here, HD), jnp.int32),
        ),
        in_specs=[smem] * 3 + [vmem] * 3 + [hbm] * 3,
        out_specs=(vmem, vmem),
        scratch_shapes=scratch + sems,
        compiler_params=pltpu.CompilerParams(
            collective_id=0, has_side_effects=True, vmem_limit_bytes=GRANT
        ),
        name="chain",
    )(
        page_table,
        prefix_lengths,
        live_lengths,
        tree_parents,
        tree_keys,
        tree_values,
        queries,
        page_keys,
        page_values,
    )


def attend(query_of, keys_of, values_of, allowed, out_to, stats, lane, first):
    for k in range(KVH):
        query = jnp.concatenate([query_of(k * GROUPS + g) for g in range(GROUPS)], axis=0)
        scores = (
            lax.dot_general(query, keys_of(k), NT, preferred_element_type=jnp.float32) * SCALE
        )
        scores = jnp.where(allowed, scores, NEG_BIG)
        peak = jnp.max(scores, axis=-1, keepdims=True)
        expo = jnp.exp(scores - peak)
        total = jnp.sum(expo, axis=-1, keepdims=True)
        out = jnp.dot(
            expo.astype(jnp.bfloat16), values_of(k), preferred_element_type=jnp.float32
        )
        rows = out.shape[0] // GROUPS
        for g in range(GROUPS):
            h = k * GROUPS + g
            part = slice(g * rows, (g + 1) * rows)
            out_to(h, out[part])
            stats = jnp.where(lane == first + h, peak[part], stats)
            stats = jnp.where(lane == first + QH + h, total[part], stats)
    return stats


def exchange(
    n,
    cap,
    table,
    prefix,
    live,
    parents_ref,
    q_ref,
    tk_ref,
    tv_ref,
    pk_hbm,
    pv_hbm,
    attended,
    reads_ref,
    pk_ref,
    pv_ref,
    target,
    used,
    label_ref,
    labels,
    label_now,
    got_out,
    got_stats,
    tree_out,
    tree_stats,
    q_all,
    q_now,
    out_send,
    stats_send,
    label_send_sem,
    label_recv_sem,
    q_send_sem,
    q_recv_sem,
    out_send_sem,
    out_recv_sem,
    stats_send_sem,
    stats_recv_sem,
    local_sem,
):
    reqs, tree, _ = q_ref.shape
    pages_here, page, _ = pk_ref.shape
    slots = table.shape[1]
    lanes = cap * 2 * QH
    fold = HD // lanes
    rows_held = tree // fold
    depth = n // 2
    me = lax.axis_index("pages")
    z, y = me // 2, me % 2
    other = 1 - y
    partner = z * 2 + other

    load_keys = pltpu.make_async_copy(pk_hbm, pk_ref, local_sem.at[2])
    load_values = pltpu.make_async_copy(pv_hbm, pv_ref, local_sem.at[3])
    load_keys.start()
    load_values.start()

    barrier = pltpu.get_barrier_semaphore()

    def greet(i, _):
        pl.semaphore_signal(
            barrier, inc=1, device_id={"pages": (me + i) % n}, device_id_type=MESH
        )
        return 0

    lax.fori_loop(1, n, greet, 0)
    pl.semaphore_wait(barrier, n - 1)

    def q_copy(src_ref, src, i, way, to):
        return pltpu.make_async_remote_copy(
            src_ref=src_ref,
            dst_ref=q_all.at[src, i],
            send_sem=q_send_sem.at[way, src // 2, i],
            recv_sem=q_recv_sem.at[src, i],
            device_id={"pages": to},
            device_id_type=MESH,
        )

    def out_copy(d):
        return pltpu.make_async_remote_copy(
            src_ref=out_send.at[d],
            dst_ref=got_out.at[pl.ds(me * cap, cap)],
            send_sem=out_send_sem.at[d],
            recv_sem=out_recv_sem.at[me],
            device_id={"pages": d},
            device_id_type=MESH,
        )

    def stats_copy(d):
        return pltpu.make_async_remote_copy(
            src_ref=stats_send.at[d],
            dst_ref=got_stats.at[me],
            send_sem=stats_send_sem.at[d],
            recv_sem=stats_recv_sem.at[me],
            device_id={"pages": d},
            device_id_type=MESH,
        )

    def q_arrive(src, i):
        pltpu.make_async_remote_copy(
            src_ref=q_all.at[src, i],
            dst_ref=q_all.at[src, i],
            send_sem=q_send_sem.at[0, src // 2, i],
            recv_sem=q_recv_sem.at[src, i],
            device_id={"pages": partner},
            device_id_type=MESH,
        ).wait_recv()

    for i in range(reqs):
        q_copy(q_ref.at[i], me, i, 2, partner).start()

        @pl.when(z + 1 < depth)
        def _():
            q_copy(q_ref.at[i], me, i, 0, me + 2).start()

        @pl.when(z > 0)
        def _():
            q_copy(q_ref.at[i], me, i, 1, me - 2).start()

    label_row = lax.broadcasted_iota(jnp.int32, (n, HD), 0)
    label_lane = lax.broadcasted_iota(jnp.int32, (n, HD), 1)
    told = jnp.zeros((n, HD), jnp.int32)
    owners, taken = [], []
    for p in range(reqs * slots):
        r, j = p // slots, p % slots
        count = jnp.clip(prefix[r] - j * page, 0, page)
        owner = lax.div(table[r, j], jnp.int32(pages_here))
        rank = jnp.int32(0)
        for earlier in range(p):
            same = (owners[earlier] == owner) & (taken[earlier] > 0)
            rank = rank + jnp.where(same, 1, 0)
        takes = jnp.where(count > 0, 1, 0)
        owners.append(owner)
        taken.append(takes)
        used[p] = takes
        target[p] = jnp.where(count > 0, owner * cap + rank, me * cap)
        row = label_row == jnp.where(count > 0, owner, -1)
        facts = (table[r, j] - owner * pages_here, count, r, live[r])
        for f, fact in enumerate(facts):
            told = jnp.where(row & (label_lane == rank * 4 + f), fact, told)
    for d in range(n):
        label_ref[d, 0:1, :] = told[d : d + 1]

    def label_copy(d):
        return pltpu.make_async_remote_copy(
            src_ref=label_ref.at[d],
            dst_ref=labels.at[me],
            send_sem=label_send_sem.at[d],
            recv_sem=label_recv_sem.at[me],
            device_id={"pages": d},
            device_id_type=MESH,
        )

    def tell(i, _):
        label_copy((me + i) % n).start()
        return 0

    lax.fori_loop(1, n, tell, 0)

    lane = lax.broadcasted_iota(jnp.int32, (tree, HD), 1)
    key_lane = lax.broadcasted_iota(jnp.int32, (GROUPS * tree, page), 1)

    def serve(d):
        stats = jnp.zeros((tree, HD), jnp.float32)
        for c in range(cap):
            which, count, req = (label_now[d, 0, c * 4 + f] for f in range(3))

            def out_to(h, value):
                out_send[d, c, :, head(h)] = value.astype(jnp.bfloat16)

            stats = attend(
                lambda h: q_now[req, :, head(h)],
                lambda k: pk_ref[which, :, head(k)],
                lambda k: pv_ref[which, :, head(k)],
                key_lane < count,
                out_to,
                stats,
                lane,
                c * 2 * QH,
            )
        stats_send[d] = jnp.concatenate(
            [stats[i * rows_held : (i + 1) * rows_held, :lanes] for i in range(fold)], axis=1
        )

    def one_tree(r, _):
        source = lax.broadcasted_iota(jnp.int32, (tree, tree), 0)
        child = lax.broadcasted_iota(jnp.int32, (tree, tree), 1)
        linked = (source == parents_ref[pl.ds(r, 1), :]) | (source == child)
        same = jnp.where(source == child, 1.0, 0.0).astype(jnp.bfloat16)
        reach = jnp.where(linked, 1.0, 0.0).astype(jnp.bfloat16)
        for level in range((tree - 1).bit_length()):
            reach = jnp.where(
                jnp.dot(reach, reach, preferred_element_type=jnp.float32) > 0, 1.0, 0.0
            ).astype(jnp.bfloat16)
        upright = lax.dot_general(
            reach, same, (((0,), (0,)), ((), ())), preferred_element_type=jnp.float32
        )
        open_ = jnp.where(child < live[r], upright, 0.0)
        allowed = jnp.concatenate([open_] * GROUPS, axis=0) > 0

        def out_to(h, value):
            tree_out[r, :, head(h)] = value

        tree_stats[r] = attend(
            lambda h: q_ref[r, :, head(h)],
            lambda k: tk_ref[r, :, head(k)],
            lambda k: tv_ref[r, :, head(k)],
            allowed,
            out_to,
            jnp.zeros((tree, HD), jnp.float32),
            lane,
            0,
        )
        return 0

    lax.fori_loop(0, reqs, one_tree, 0)

    labels[me] = label_ref[me]

    def hear(i, _):
        d = (me + i) % n
        pltpu.make_async_remote_copy(
            src_ref=label_ref.at[d],
            dst_ref=labels.at[d],
            send_sem=label_send_sem.at[d],
            recv_sem=label_recv_sem.at[d],
            device_id={"pages": d},
            device_id_type=MESH,
        ).wait()
        return 0

    lax.fori_loop(1, n, hear, 0)
    into_scalars = pltpu.make_async_copy(labels, label_now, local_sem.at[0])
    into_scalars.start()
    into_scalars.wait()
    load_keys.wait()
    load_values.wait()

    q_now[...] = q_ref[...]
    serve(me)
    for c in range(cap):
        got_out[me * cap + c] = out_send[me, c]
    got_stats[me] = stats_send[me]

    page_row = lax.broadcasted_iota(jnp.int32, (pages_here, HD), 0)

    def count_reads(d, reads):
        for c in range(cap):
            which, count, _, lives = (label_now[d, 0, c * 4 + f] for f in range(4))
            lives = jnp.where(count > 0, lives, 0)
            reads = reads + jnp.where(page_row == which, lives, 0)
        return reads

    reads_ref[...] = lax.fori_loop(
        0, n, count_reads, jnp.zeros((pages_here, HD), jnp.int32)
    )

    def step(s, _):
        for i in range(reqs):

            @pl.when(z - s >= 0)
            def _():
                src = me - 2 * s
                q_arrive(src, i)
                q_copy(q_all.at[src, i], src, i, 2, partner).start()

                @pl.when(z + 1 < depth)
                def _():
                    q_copy(q_all.at[src, i], src, i, 0, me + 2).start()

            @pl.when(z + s < depth)
            def _():
                src = me + 2 * s
                q_arrive(src, i)
                q_copy(q_all.at[src, i], src, i, 2, partner).start()

                @pl.when(z > 0)
                def _():
                    q_copy(q_all.at[src, i], src, i, 1, me - 2).start()

        def case(k, _):
            crossed = k // 2
            far = s - crossed
            row = z + far * (2 * (k % 2) - 1)
            column = y + crossed * (other - y)
            d = row * 2 + column
            valid = (row >= 0) & (row < depth) & ((far > 0) | (k == 2))

            @pl.when(valid)
            def _():
                @pl.when(crossed == 1)
                def _():
                    for i in range(reqs):
                        q_arrive(d, i)

                q_now[...] = q_all[d]
                serve(d)
                out_copy(d).start()
                stats_copy(d).start()

            return 0

        lax.fori_loop(0, 4, case, 0)
        return 0

    lax.fori_loop(1, depth + 1, step, 0)

    def finish(i, _):
        d = (me + i) % n
        out_copy(d).wait_send()
        stats_copy(d).wait_send()
        pltpu.make_async_remote_copy(
            src_ref=out_send.at[d],
            dst_ref=got_out.at[pl.ds(d * cap, cap)],
            send_sem=out_send_sem.at[d],
            recv_sem=out_recv_sem.at[d],
            device_id={"pages": d},
            device_id_type=MESH,
        ).wait_recv()
        pltpu.make_async_remote_copy(
            src_ref=stats_send.at[d],
            dst_ref=got_stats.at[d],
            send_sem=stats_send_sem.at[d],
            recv_sem=stats_recv_sem.at[d],
            device_id={"pages": d},
            device_id_type=MESH,
        ).wait_recv()
        return 0

    lax.fori_loop(1, n, finish, 0)

    def drain(row, _):
        src = row * 2 + y
        for i in range(reqs):
            q_copy(q_all.at[src, i], src, i, 2, partner).wait_send()

            @pl.when((row <= z) & (z + 1 < depth))
            def _():
                q_copy(q_all.at[src, i], src, i, 0, me + 2).wait_send()

            @pl.when((row >= z) & (z > 0))
            def _():
                q_copy(q_all.at[src, i], src, i, 1, me - 2).wait_send()

        return 0

    lax.fori_loop(0, depth, drain, 0)

    def merge(r, _):
        tree_peak, tree_total = tree_stats[r, :, :QH], tree_stats[r, :, QH : 2 * QH]
        top = tree_peak
        peaks, totals = [], []
        for j in range(slots):
            where_ = target[r * slots + j]
            live_slot = used[r * slots + j] > 0
            packed = got_stats[where_ // cap]
            held = jnp.concatenate(
                [packed[:, i * lanes : (i + 1) * lanes] for i in range(fold)], axis=0
            )
            mine = held[:, : 2 * QH]
            for c in range(1, cap):
                mine = jnp.where(
                    where_ % cap == c, held[:, c * 2 * QH : (c + 1) * 2 * QH], mine
                )
            peaks.append(jnp.where(live_slot, mine[:, :QH], NEG_BIG))
            totals.append(mine[:, QH:])
            top = jnp.maximum(top, peaks[j])
        tree_scale = jnp.exp(tree_peak - top)
        scales = [
            jnp.where(used[r * slots + j] > 0, jnp.exp(peaks[j] - top), 0.0)
            for j in range(slots)
        ]
        total = tree_total * tree_scale
        for j in range(slots):
            total = total + scales[j] * totals[j]
        tree_scale = tree_scale / total
        scales = [scale / total for scale in scales]
        for h in range(QH):
            mixed = tree_out[r, :, head(h)] * tree_scale[:, h : h + 1]
            for j in range(slots):
                part = got_out[target[r * slots + j], :, head(h)].astype(jnp.float32)
                mixed = mixed + part * scales[j][:, h : h + 1]
            attended[r, :, head(h)] = mixed.astype(jnp.bfloat16)
        return 0

    lax.fori_loop(0, reqs, merge, 0)


def shards(
    queries,
    tree_keys,
    tree_values,
    page_keys,
    page_values,
    page_table,
    prefix_lengths,
    tree_parents,
    live_lengths,
):
    n = lax.axis_size("pages")
    reqs, tree, width = queries.shape
    pages_here = page_keys.shape[0]
    slots = page_table.shape[1]
    pairs = reqs * slots
    cap = max(1, pairs // n)
    args = (queries, tree_keys, tree_values, page_keys, page_values)
    args += (page_table, prefix_lengths, tree_parents, live_lengths)
    if 7 * n * reqs * tree * width < GRANT:
        attended, reads = chain_call(n, cap, args)
        return attended, reads[:, 0]

    smem = pl.BlockSpec(memory_space=pltpu.SMEM)
    vmem = pl.BlockSpec(memory_space=pltpu.VMEM)
    hbm = pl.BlockSpec(memory_space=pl.ANY)
    depth = n // 2
    held_stats = (n, tree * cap * 2 * QH // HD, HD)
    attended, reads = pl.pallas_call(
        functools.partial(exchange, n, cap),
        out_shape=(
            jax.ShapeDtypeStruct((reqs, tree, width), jnp.bfloat16),
            jax.ShapeDtypeStruct((pages_here, HD), jnp.int32),
        ),
        in_specs=[smem] * 3 + [vmem] * 4 + [hbm] * 2,
        out_specs=(vmem, vmem),
        scratch_shapes=[
            pltpu.VMEM(page_keys.shape, jnp.bfloat16),
            pltpu.VMEM(page_values.shape, jnp.bfloat16),
            pltpu.SMEM((pairs,), jnp.int32),
            pltpu.SMEM((pairs,), jnp.int32),
            pltpu.VMEM((n, 8, HD), jnp.int32),
            pltpu.VMEM((n, 8, HD), jnp.int32),
            pltpu.SMEM((n, 8, HD), jnp.int32),
            pltpu.VMEM((n * cap, tree, width), jnp.bfloat16),
            pltpu.VMEM(held_stats, jnp.float32),
            pltpu.VMEM((reqs, tree, width), jnp.float32),
            pltpu.VMEM((reqs, tree, HD), jnp.float32),
            pltpu.VMEM((n, reqs, tree, width), jnp.bfloat16),
            pltpu.VMEM((reqs, tree, width), jnp.bfloat16),
            pltpu.VMEM((n, cap, tree, width), jnp.bfloat16),
            pltpu.VMEM(held_stats, jnp.float32),
            pltpu.SemaphoreType.DMA((n,)),
            pltpu.SemaphoreType.DMA((n,)),
            pltpu.SemaphoreType.DMA((3, depth, reqs)),
            pltpu.SemaphoreType.DMA((n, reqs)),
            pltpu.SemaphoreType.DMA((n,)),
            pltpu.SemaphoreType.DMA((n,)),
            pltpu.SemaphoreType.DMA((n,)),
            pltpu.SemaphoreType.DMA((n,)),
            pltpu.SemaphoreType.DMA((4,)),
        ],
        compiler_params=pltpu.CompilerParams(
            collective_id=0, has_side_effects=True, vmem_limit_bytes=63 * 1024 * 1024
        ),
        name="exchange",
    )(
        page_table,
        prefix_lengths,
        live_lengths,
        tree_parents,
        queries,
        tree_keys,
        tree_values,
        page_keys,
        page_values,
    )
    return (attended, reads[:, 0])


def solution(mesh):
    rows = P(("grp", "pages"), None, None)
    return jax.shard_map(
        shards,
        mesh=mesh,
        in_specs=(
            rows,
            rows,
            rows,
            rows,
            rows,
            P(("grp", "pages"), None),
            P(("grp", "pages")),
            P(("grp", "pages"), None),
            P(("grp", "pages")),
        ),
        out_specs=(rows, P(("grp", "pages"))),
        check_vma=False,
    )
```
